512 devices in a mesh: trial: 4 (over x), span: 16 (over y, core), heads: 8 (over z).
Axes of the slice: x: 4, y: 8, z: 8, core: 2. Of those that a mesh axis runs over, the one named last changes fastest.
Arguments:
- latents: bfloat16 [64, 4096, 512], P('trial', ('span', 'heads')), parts along dimension 0, may hold values from -6 to 6
- rotary_rows: bfloat16 [64, 4096, 64], P('trial', ('span', 'heads')), parts along dimension 0, may hold values from -6 to 6
- latent_gain: float32 [512], replicated, may hold values from 0.25 to 1.75
- key_up: bfloat16 [2048, 16, 128], P('trial', 'heads'), parts along dimension 0, may hold values from -0.25 to 0.25
- value_up: bfloat16 [2048, 16, 128], P('trial', 'heads'), parts along dimension 0, may hold values from -0.25 to 0.25
Outputs:
- cache_keys: bfloat16 [64, 16, 192, 4096], P(('trial', 'span'), 'heads'), parts along dimension 0
- cache_values: bfloat16 [64, 4096, 16, 128], P(('trial', 'span'), None, 'heads'), parts along dimension 0
The draws below stay inside these ranges and needn't reach their ends.
There are 4 independent parts, one for each index of `trial`. The reference program is written for one: setup_inputs(seed, part) draws one part's arguments, and reference() takes and returns one part's arrays. A program takes and returns all parts, laid end to end along the dimension named above; an argument that names none is the same for every part. Nothing has to cross between parts.
All inputs are finite; a program needn't handle non-finite values.
Results may differ from the reference program's by a relative error of at most 0.0049.
Values may be sent and summed in bfloat16 or wider, within the bound.
A program may use at most 64 MiB of HBM per device.

```python
import jax
import jax.numpy as jnp
from jax import lax

BATCH = 16
LENGTH = 4096
HEADS = 16
LATENT = 512
KEY_PART = 128
ROTARY = 64
VALUE_SIZE = 128


def shard_levels(key, extent, shards, smallest, high):
    level, own = 1.0, jax.random.fold_in(key, 6)
    for dim, blocks in shards:
        steps = jnp.exp(jax.random.uniform(jax.random.fold_in(own, dim), (blocks,), jnp.float32, smallest / len(shards), high / len(shards)))
        level = level * jnp.repeat(steps, extent[dim] // blocks).reshape([-1 if axis == dim else 1 for axis in range(len(extent))])
    return level


def bell_draw(own_key, shape, width, most, cuts=(), kind=jnp.bfloat16):
    values = width * jax.random.normal(own_key, shape, jnp.float32)
    if cuts:
        values = values * shard_levels(own_key, shape, cuts, -0.22, 0.18)
    return jnp.clip(values, -most, most).astype(kind)


def setup_inputs(seed: int = 0, part: int = 0) -> dict:
    seeds = jax.random.split(jax.random.key(seed), 6)
    own_keys = jax.random.split(jax.random.fold_in(seeds[5], part), 6)
    return {
        "latents": bell_draw(own_keys[0], (BATCH, LENGTH, LATENT), 1.0, 6.0, ((1, 128),)),
        "rotary_rows": bell_draw(own_keys[1], (BATCH, LENGTH, ROTARY), 1.0, 6.0, ((1, 128),)),
        "latent_gain": jnp.clip(1.0 + 0.15 * jax.random.normal(seeds[2], (LATENT,), jnp.float32), 0.25, 1.75),
        "key_up": bell_draw(own_keys[3], (LATENT, HEADS, KEY_PART), LATENT ** -0.5, 0.25, ((1, 8),)),
        "value_up": bell_draw(own_keys[4], (LATENT, HEADS, VALUE_SIZE), LATENT ** -0.5, 0.25, ((1, 8),)),
    }


def unit_rows(vectors, row_gain):
    return vectors * lax.rsqrt(lax.optimization_barrier(jnp.mean(vectors * vectors, axis=-1, keepdims=True)) + 1e-06) * row_gain

def reference(latents, rotary_rows, latent_gain, key_up, value_up):
    rows_ready = unit_rows(latents.astype(jnp.float32), latent_gain).astype(jnp.bfloat16)
    rows_ready = lax.optimization_barrier(rows_ready)

    def expand_one(one):
        rows_one, rotary_one = one
        wide_keys = jnp.einsum('tr,rhk->thk', rows_one.astype(jnp.float32), key_up.astype(jnp.float32)).astype(jnp.bfloat16)
        shared = jnp.broadcast_to(rotary_one[:, None], (LENGTH, HEADS, ROTARY))
        wide_values = jnp.einsum('tr,rhk->thk', rows_one.astype(jnp.float32), value_up.astype(jnp.float32)).astype(jnp.bfloat16)
        return (jnp.concatenate([wide_keys, shared], axis=-1), wide_values)
    cache_keys, cache_values = lax.map(expand_one, (rows_ready, rotary_rows))
    cache_keys = jnp.transpose(cache_keys, (0, 2, 3, 1))
    return (cache_keys, cache_values)
```

```python
import functools

import jax
import jax.numpy as jnp
from jax import lax
from jax.experimental import pallas as pl
from jax.experimental.pallas import tpu as pltpu
from jax.sharding import PartitionSpec as P

MESH = pl.DeviceIdType.MESH
BF16, F32 = jnp.bfloat16, jnp.float32

SPANS, RING = 16, 8
COUNT, DEPTH = 32, 512
TURN, WIDTH = 64, 128
TILES = 8
BATCH = 4


def widen_rows(rows, rotary, key_up, value_up):
    wide_keys = jnp.einsum(
        "btr,rhk->bthk", rows, key_up, preferred_element_type=jnp.float32
    ).astype(jnp.bfloat16)
    shared = jnp.broadcast_to(rotary[:, :, None], wide_keys.shape[:3] + rotary.shape[2:])
    wide_values = jnp.einsum(
        "btr,rhk->bthk", rows, value_up, preferred_element_type=jnp.float32
    ).astype(jnp.bfloat16)
    return (jnp.concatenate([wide_keys, shared], axis=-1), wide_values)


def unit_rows(vectors, row_gain):
    return (
        vectors * lax.rsqrt(jnp.mean(vectors * vectors, axis=-1, keepdims=True) + 1e-06) * row_gain
    )


def plain_shards(latents, rotary_rows, latent_gain, key_up, value_up):
    rows_ready = unit_rows(latents.astype(jnp.float32), latent_gain).astype(jnp.bfloat16)

    def move(block):
        block = lax.all_to_all(block, "span", split_axis=0, concat_axis=1, tiled=True)
        block = block.reshape(block.shape[0], lax.axis_size("span"), -1, block.shape[2])
        block = lax.all_gather(block, "heads", axis=2, tiled=True)
        return block.reshape(block.shape[0], -1, block.shape[3])

    cache_keys, cache_values = widen_rows(move(rows_ready), move(rotary_rows), key_up, value_up)
    return (jnp.transpose(cache_keys, (0, 2, 3, 1)), cache_values)


def source(me, k):
    j, flip = k // 2, k % 2
    away = ((j + 1) // 2) * (2 * (j % 2) - 1)
    core = (me % 2) * (1 - 2 * flip) + flip
    return ((me // 2 + away + SPANS // 2) % (SPANS // 2)) * 2 + core


def target(me, k):
    j, flip = k // 2, k % 2
    away = ((j + 1) // 2) * (2 * (j % 2) - 1)
    core = (me % 2) * (1 - 2 * flip) + flip
    return ((me // 2 - away + SPANS // 2) % (SPANS // 2)) * 2 + core


def exchange_kernel(
    lat, rot, far_gain, key_up, value_up, keys, values,
    buf, stage, rot_raw, raw_w, key_wide, value_wide, gain, pick, flat,
    load_sem, y_send, y_recv, z_send, z_recv,
):
    me, z = lax.axis_index("span"), lax.axis_index("heads")
    ahead, behind = lax.rem(z + 1, RING), lax.rem(z + RING - 1, RING)

    barrier = pltpu.get_barrier_semaphore()
    for near in (ahead, behind):
        pl.semaphore_signal(barrier, inc=1, device_id={"heads": near}, device_id_type=MESH)
    for k in range(1, SPANS):
        pl.semaphore_signal(barrier, inc=1, device_id={"span": target(me, k)}, device_id_type=MESH)

    rot_load = pltpu.make_async_copy(rot, rot_raw, load_sem.at[0])
    rot_load.start()
    loads = []
    for t in range(TILES):
        rows = pl.ds(16 * (t // 4), 16)
        columns = pl.ds(128 * (t % 4), 128)
        loads.append(pltpu.make_async_copy(
            lat.at[:, rows, columns], stage.at[:, t], load_sem.at[1 + t]
        ))
    weights = [
        pltpu.make_async_copy(key_up, raw_w.at[0], load_sem.at[9]),
        pltpu.make_async_copy(value_up, raw_w.at[1], load_sem.at[10]),
        pltpu.make_async_copy(far_gain, gain, load_sem.at[11]),
    ]
    for copy in (*loads, *weights):
        copy.start()
    rot_load.wait()

    @pl.loop(0, SPANS)
    def _(s):
        part = rot_raw[s].astype(F32)
        stage[s, TILES] = jnp.concatenate([part[:16], part[16:]], axis=1).astype(BF16)

    for copy in loads:
        copy.wait()
    pl.semaphore_wait(barrier, SPANS + 1)

    def z_copy(way, d, k):
        if way == 0:
            here, there, to = (RING + 1 - d) % RING, RING - d, ahead
        else:
            here, there, to = d - 1, d, behind
        src = stage.at[me] if (d == 1 and k == 0) else buf.at[here, k]
        n = (way * 4 + d - 1) * SPANS + k
        return pltpu.make_async_remote_copy(
            src_ref=src, dst_ref=buf.at[there, k], send_sem=z_send.at[n], recv_sem=z_recv.at[n],
            device_id={"heads": to}, device_id_type=MESH,
        )

    def y_copy(k):
        to = target(me, k)
        return pltpu.make_async_remote_copy(
            src_ref=stage.at[to], dst_ref=buf.at[0, k], send_sem=y_send.at[k], recv_sem=y_recv.at[k],
            device_id={"span": to}, device_id_type=MESH,
        )

    heard = set()

    def need(way, d, k):
        if d == 0:
            if k and (0, k) not in heard:
                heard.add((0, k))
                y_copy(k).wait_recv()
        elif (way, d, k) not in heard:
            heard.add((way, d, k))
            z_copy(way, d, k).wait_recv()

    def last_way(k):
        return k % 2

    sent = []

    def forward(d, ks):
        for k in ks:
            for way in (0, 1):
                need(way, d - 1, k)
                if d < 4 or way == last_way(k):
                    z_copy(way, d, k).start()
                    sent.append((way, d, k))

    forward(1, [0])
    for k in range(1, SPANS):
        y_copy(k).start()
    buf[0, 0] = stage[me]

    for copy in weights:
        copy.wait()
    for w, put in ((0, key_wide), (1, value_wide)):
        @pl.loop(0, 4)
        def _(n):
            r = pl.multiple_of(n * 256, 256)
            flat[...] = raw_w[w, pl.ds(r, 256), :].astype(F32)
            at = pl.multiple_of(n * 128, 128)
            for h in range(2):
                block = flat[pl.ds(h, 128, stride=2), :]
                if w == 0:
                    key_wide[h * WIDTH:(h + 1) * WIDTH, pl.ds(at, 128)] = block.T.astype(BF16)
                else:
                    value_wide[pl.ds(at, 128), h * WIDTH:(h + 1) * WIDTH] = block.astype(BF16)
    row = lax.broadcasted_iota(jnp.int32, (64, 128), 0)
    column = lax.broadcasted_iota(jnp.int32, (64, 128), 1)
    for half in range(2):
        place = (row // 16) * 32 + half * 16 + row % 16
        pick[half] = jnp.where(place == column, 1.0, 0.0).astype(BF16)

    def expand(k, other):
        group = z // 4 if not other else 1 - z // 4
        start = pl.multiple_of(source(me, k) * 256 + group * 128, 128)
        rows, turned = [], []
        for zz in range(4):
            rel = lax.rem(group * 4 + zz + RING - z, RING)
            for half in range(2):
                raw = jnp.concatenate(
                    [buf[rel, k, half * 4 + c].astype(F32) for c in range(4)], axis=1
                )
                rows.append(unit_rows(raw, gain[...]).astype(BF16))
            turned.append(buf[rel, k, TILES])
        ready = jnp.concatenate(rows, axis=0)
        turned = jnp.concatenate(turned, axis=0)
        wide = lax.dot_general(
            key_wide[...], ready, (((1,), (1,)), ((), ())), preferred_element_type=F32
        ).astype(BF16)
        halves = [
            lax.dot_general(turned, pick[half], (((0,), (0,)), ((), ())), preferred_element_type=F32)
            for half in range(2)
        ]
        shared = (halves[0][:TURN] + halves[1][TURN:]).astype(BF16)
        for h in range(2):
            keys[h, :WIDTH, pl.ds(start, 128)] = wide[h * WIDTH:(h + 1) * WIDTH]
            keys[h, WIDTH:, pl.ds(start, 128)] = shared
        wide = jnp.dot(ready, value_wide[...], preferred_element_type=F32)
        for h in range(2):
            flat[pl.ds(h, 128, stride=2), :] = wide[:, h * WIDTH:(h + 1) * WIDTH]
        values[pl.ds(pl.multiple_of(start * 2, 256), 256), :] = flat[...].astype(BF16)

    def compute(other, b):
        ks = batch(b)
        for k in ks:
            for way in (0, 1):
                need(way, 3, k)
            if other:
                need(last_way(k), 4, k)
        for k in ks:
            assert (0, k) in heard or k == 0

        @pl.loop(ks[0], ks[-1] + 1)
        def _(k):
            expand(k, other)

    def batch(b):
        return list(range(b * BATCH, (b + 1) * BATCH))

    forward(1, batch(0)[1:])
    forward(1, batch(1))
    forward(2, batch(0))
    forward(1, batch(2))
    forward(2, batch(1))
    forward(3, batch(0))
    forward(1, batch(3))
    forward(2, batch(2))
    forward(4, batch(0))
    forward(3, batch(1))
    compute(False, 0)
    forward(2, batch(3))
    compute(True, 0)
    forward(4, batch(1))
    forward(3, batch(2))
    compute(False, 1)
    forward(3, batch(3))
    compute(True, 1)
    forward(4, batch(2))
    compute(False, 2)
    forward(4, batch(3))
    compute(False, 3)
    compute(True, 2)
    compute(True, 3)

    for k in range(1, SPANS):
        y_copy(k).wait_send()
    for way, d, k in sent:
        z_copy(way, d, k).wait_send()


def write_kernel(keys_part, values_part, keys, values, sem):
    copies = []
    for h in range(2):
        for n in range(2):
            rows = pl.ds(96 * n, 96)
            copies.append(pltpu.make_async_copy(
                keys_part.at[h, rows], keys.at[0, h, rows], sem.at[len(copies)]
            ))
    for n in range(4):
        rows = pl.ds(2048 * n, 2048)
        copies.append(pltpu.make_async_copy(
            values_part.at[rows], values.at[rows], sem.at[len(copies)]
        ))
    for copy in copies:
        copy.start()
    for copy in copies:
        copy.wait()


def shards(latents, rotary_rows, latent_gain, key_up, value_up):
    shape = (lax.axis_size("span"), lax.axis_size("heads"), *latents.shape, rotary_rows.shape[2])
    if shape != (SPANS, RING, SPANS, COUNT, DEPTH, TURN) or key_up.shape != (DEPTH, 2, WIDTH) or (
        value_up.shape != (DEPTH, 2, WIDTH)
    ):
        return plain_shards(latents, rotary_rows, latent_gain, key_up, value_up)
    length = SPANS * RING * COUNT
    near = pl.BlockSpec(memory_space=pltpu.VMEM)
    far = pl.BlockSpec(memory_space=pltpu.HBM)
    args = (
        latents, rotary_rows, latent_gain[None],
        key_up.reshape(2 * DEPTH, WIDTH), value_up.reshape(2 * DEPTH, WIDTH),
    )
    parts = pl.pallas_call(
        exchange_kernel,
        out_shape=(
            pltpu.VMEM((2, WIDTH + TURN, length), BF16),
            pltpu.VMEM((2 * length, WIDTH), BF16),
        ),
        in_specs=[far] * 5,
        out_specs=[near] * 2,
        scratch_shapes=[
            pltpu.VMEM((RING, SPANS, TILES + 1, 16, 128), BF16),
            pltpu.VMEM((SPANS, TILES + 1, 16, 128), BF16),
            pltpu.VMEM((SPANS, COUNT, TURN), BF16),
            pltpu.VMEM((2, 2 * DEPTH, WIDTH), BF16),
            pltpu.VMEM((2 * WIDTH, DEPTH), BF16),
            pltpu.VMEM((DEPTH, 2 * WIDTH), BF16),
            pltpu.VMEM((1, DEPTH), F32),
            pltpu.VMEM((2, 64, 128), BF16),
            pltpu.VMEM((256, WIDTH), F32),
            pltpu.SemaphoreType.DMA((12,)),
            pltpu.SemaphoreType.DMA((SPANS,)),
            pltpu.SemaphoreType.DMA((SPANS,)),
            pltpu.SemaphoreType.DMA((8 * SPANS,)),
            pltpu.SemaphoreType.DMA((8 * SPANS,)),
        ],
        compiler_params=pltpu.CompilerParams(
            collective_id=0, has_side_effects=True, vmem_limit_bytes=40 * 1024 * 1024
        ),
    )(*(pltpu.with_memory_space_constraint(arg, pltpu.HBM) for arg in args))
    keys, values = pl.pallas_call(
        write_kernel,
        out_shape=(
            jax.ShapeDtypeStruct((1, 2, WIDTH + TURN, length), BF16),
            jax.ShapeDtypeStruct((2 * length, WIDTH), BF16),
        ),
        in_specs=[near] * 2,
        out_specs=[far] * 2,
        scratch_shapes=[pltpu.SemaphoreType.DMA((8,))],
        compiler_params=pltpu.CompilerParams(vmem_limit_bytes=16 * 1024 * 1024),
    )(*parts)
    return keys, values.reshape(1, length, 2, WIDTH)


def solution(mesh):
    return jax.shard_map(
        shards,
        mesh=mesh,
        in_specs=(
            P("trial", ("span", "heads"), None),
            P("trial", ("span", "heads"), None),
            P(),
            P("trial", "heads", None),
            P("trial", "heads", None),
        ),
        out_specs=(
            P(("trial", "span"), "heads", None, None),
            P(("trial", "span"), None, "heads", None),
        ),
        check_vma=False,
    )
```

```python
import functools

import jax
import jax.numpy as jnp
from jax import lax
from jax.experimental import pallas as pl
from jax.experimental.pallas import tpu as pltpu
from jax.sharding import PartitionSpec as P

MESH = pl.DeviceIdType.MESH
BF16, F32 = jnp.bfloat16, jnp.float32

SPANS, RING = 16, 8
COUNT, DEPTH = 32, 512
TURN, WIDTH = 64, 128
TILES = 8


def widen_rows(rows, rotary, key_up, value_up):
    wide_keys = jnp.einsum(
        "btr,rhk->bthk", rows, key_up, preferred_element_type=jnp.float32
    ).astype(jnp.bfloat16)
    shared = jnp.broadcast_to(rotary[:, :, None], wide_keys.shape[:3] + rotary.shape[2:])
    wide_values = jnp.einsum(
        "btr,rhk->bthk", rows, value_up, preferred_element_type=jnp.float32
    ).astype(jnp.bfloat16)
    return (jnp.concatenate([wide_keys, shared], axis=-1), wide_values)


def unit_rows(vectors, row_gain):
    return (
        vectors * lax.rsqrt(jnp.mean(vectors * vectors, axis=-1, keepdims=True) + 1e-06) * row_gain
    )


def plain_shards(latents, rotary_rows, latent_gain, key_up, value_up):
    rows_ready = unit_rows(latents.astype(jnp.float32), latent_gain).astype(jnp.bfloat16)

    def move(block):
        block = lax.all_to_all(block, "span", split_axis=0, concat_axis=1, tiled=True)
        block = block.reshape(block.shape[0], lax.axis_size("span"), -1, block.shape[2])
        block = lax.all_gather(block, "heads", axis=2, tiled=True)
        return block.reshape(block.shape[0], -1, block.shape[3])

    cache_keys, cache_values = widen_rows(move(rows_ready), move(rotary_rows), key_up, value_up)
    return (jnp.transpose(cache_keys, (0, 2, 3, 1)), cache_values)


def source(me, k):
    j, flip = k // 2, k % 2
    away = ((j + 1) // 2) * (2 * (j % 2) - 1)
    core = (me % 2) * (1 - 2 * flip) + flip
    return ((me // 2 + away + SPANS // 2) % (SPANS // 2)) * 2 + core


def target(me, k):
    j, flip = k // 2, k % 2
    away = ((j + 1) // 2) * (2 * (j % 2) - 1)
    core = (me % 2) * (1 - 2 * flip) + flip
    return ((me // 2 - away + SPANS // 2) % (SPANS // 2)) * 2 + core


def exchange_kernel(
    lat, rot, far_gain, key_up, value_up, keys, values,
    buf, stage, rot_raw, raw_w, key_wide, value_wide, gain, pick, flat,
    ready, load_sem, y_send, y_recv, z_send, z_recv,
):
    me, z = lax.axis_index("span"), lax.axis_index("heads")
    ahead, behind = lax.rem(z + 1, RING), lax.rem(z + RING - 1, RING)

    barrier = pltpu.get_barrier_semaphore()
    sibling = target(me, 1)
    greeted = [{"heads": ahead}, {"heads": behind}, {"span": sibling}]
    greeted += [{"span": sibling, "heads": ahead}, {"span": sibling, "heads": behind}]
    greeted += [{"span": target(me, k)} for k in range(2, 6)]
    for near in greeted:
        pl.semaphore_signal(barrier, inc=1, device_id=near, device_id_type=MESH)

    rot_load = pltpu.make_async_copy(rot, rot_raw, load_sem.at[0])
    rot_load.start()
    loads = []
    for t in range(TILES):
        rows = pl.ds(16 * (t // 4), 16)
        columns = pl.ds(128 * (t % 4), 128)
        loads.append(pltpu.make_async_copy(
            lat.at[:, rows, columns], stage.at[:, t], load_sem.at[1 + t]
        ))
    weights = [
        pltpu.make_async_copy(key_up, raw_w.at[0], load_sem.at[9]),
        pltpu.make_async_copy(value_up, raw_w.at[1], load_sem.at[10]),
        pltpu.make_async_copy(far_gain, gain, load_sem.at[11]),
    ]
    for copy in (*loads, *weights):
        copy.start()
    rot_load.wait()

    @pl.loop(0, SPANS)
    def _(s):
        part = rot_raw[s].astype(F32)
        stage[s, TILES] = jnp.concatenate([part[:16], part[16:]], axis=1).astype(BF16)

    for copy in loads:
        copy.wait()
    pl.semaphore_wait(barrier, len(greeted))

    def z_copy(way, d, k):
        if way == 0:
            here, there, to = (RING + 1 - d) % RING, RING - d, ahead
        else:
            here, there, to = d - 1, d, behind
        src, device = buf.at[here, k], {"heads": to}
        if d == 1 and k == 0:
            src = stage.at[me]
        if d == 1 and k == 1:
            src, device = stage.at[sibling], {"span": sibling, "heads": to}
        n = (way * 4 + d - 1) * SPANS + k
        return pltpu.make_async_remote_copy(
            src_ref=src, dst_ref=buf.at[there, k], send_sem=z_send.at[n], recv_sem=z_recv.at[n],
            device_id=device, device_id_type=MESH,
        )

    def y_copy(k):
        to = target(me, k)
        return pltpu.make_async_remote_copy(
            src_ref=stage.at[to], dst_ref=buf.at[0, k], send_sem=y_send.at[k], recv_sem=y_recv.at[k],
            device_id={"span": to}, device_id_type=MESH,
        )

    heard = set()

    def need(way, d, k):
        if d == 0:
            if k and (0, k) not in heard:
                heard.add((0, k))
                y_copy(k).wait_recv()
        elif (way, d, k) not in heard:
            heard.add((way, d, k))
            z_copy(way, d, k).wait_recv()

    def last_way(k):
        return k % 2

    sent = []

    def forward(d, ks):
        for k in ks:
            for way in (0, 1):
                if d > 1 or k > 1:
                    need(way, d - 1, k)
                if d < 4 or way == last_way(k):
                    z_copy(way, d, k).start()
                    sent.append((way, d, k))

    def spread(ks):
        for k in ks:
            y_copy(k).start()

    forward(1, [0, 1])
    spread(range(1, 6))
    buf[0, 0] = stage[me]

    for copy in weights:
        copy.wait()
    for w, put in ((0, key_wide), (1, value_wide)):
        @pl.loop(0, 4)
        def _(n):
            r = pl.multiple_of(n * 256, 256)
            flat[pl.ds(0, 256), :] = raw_w[w, pl.ds(r, 256), :].astype(F32)
            at = pl.multiple_of(n * 128, 128)
            for h in range(2):
                block = flat[pl.ds(h, 128, stride=2), :]
                if w == 0:
                    key_wide[h * WIDTH:(h + 1) * WIDTH, pl.ds(at, 128)] = block.T.astype(BF16)
                else:
                    value_wide[pl.ds(at, 128), h * WIDTH:(h + 1) * WIDTH] = block.astype(BF16)
    row = lax.broadcasted_iota(jnp.int32, (64, 128), 0)
    column = lax.broadcasted_iota(jnp.int32, (64, 128), 1)
    for half in range(2):
        place = (row // 16) * 32 + half * 16 + row % 16
        pick[half] = jnp.where(place == column, 1.0, 0.0).astype(BF16)

    def expand(p, other):
        group = z // 4 if not other else 1 - z // 4
        pair = (2 * p, 2 * p + 1)
        for k in pair:
            need(0, 0, k)
            for way in (0, 1):
                need(way, 3, k)
            if other:
                need(last_way(k), 4, k)
        rels = [lax.rem(group * 4 + zz + RING - z, RING) for zz in range(4)]
        starts = [pl.multiple_of(source(me, k) * 256 + group * 128, 128) for k in pair]
        for i, k in enumerate(pair):
            for zz in range(4):
                for half in range(2):
                    raw = jnp.concatenate(
                        [buf[rels[zz], k, half * 4 + c].astype(F32) for c in range(4)], axis=1
                    )
                    ready[pl.ds(i * 128 + zz * 32 + half * 16, 16), :] = (
                        unit_rows(raw, gain[...]).astype(BF16)
                    )
        wide = lax.dot_general(
            key_wide[...], ready[...], (((1,), (1,)), ((), ())), preferred_element_type=F32
        ).astype(BF16)
        for i, k in enumerate(pair):
            turned = jnp.concatenate([buf[rels[zz], k, TILES] for zz in range(4)], axis=0)
            halves = [
                lax.dot_general(
                    turned, pick[half], (((0,), (0,)), ((), ())), preferred_element_type=F32
                )
                for half in range(2)
            ]
            shared = (halves[0][:TURN] + halves[1][TURN:]).astype(BF16)
            for h in range(2):
                keys[h, :WIDTH, pl.ds(starts[i], 128)] = (
                    wide[h * WIDTH:(h + 1) * WIDTH, i * 128:(i + 1) * 128]
                )
                keys[h, WIDTH:, pl.ds(starts[i], 128)] = shared
        wide = jnp.dot(ready[...], value_wide[...], preferred_element_type=F32)
        for h in range(2):
            flat[pl.ds(h, 256, stride=2), :] = wide[:, h * WIDTH:(h + 1) * WIDTH]
        for i in range(2):
            at = pl.multiple_of(starts[i] * 2, 256)
            values[pl.ds(at, 256), :] = flat[pl.ds(i * 256, 256), :].astype(BF16)

    def hop(d, *pairs):
        for p in pairs:
            forward(d, [2 * p, 2 * p + 1])

    own, far = functools.partial(expand, other=False), functools.partial(expand, other=True)

    forward(2, [0])
    forward(1, [2])
    forward(2, [1])
    forward(1, [3, 4, 5])
    spread(range(6, 10))
    hop(2, 1)
    hop(1, 3, 4)
    spread(range(10, 16))
    hop(2, 2)
    hop(3, 0)
    hop(2, 3)
    hop(3, 1)
    hop(1, 5)
    hop(2, 4)
    hop(1, 6)
    hop(4, 0)
    own(0)
    hop(3, 2)
    hop(1, 7)
    own(1)
    hop(2, 5)
    hop(3, 3)
    far(0)
    hop(4, 1)
    hop(2, 6)
    hop(4, 2)
    own(2)
    hop(3, 4)
    far(1)
    hop(2, 7)
    hop(3, 5)
    own(3)
    hop(4, 3)
    hop(3, 6)
    far(2)
    hop(3, 7)
    own(4)
    hop(4, 4, 5)
    own(5)
    hop(4, 6, 7)
    for k in range(1, SPANS):
        y_copy(k).wait_send()
    early, late = sent[:-16], sent[-16:]
    for way, d, k in early:
        z_copy(way, d, k).wait_send()
    far(3)
    own(6)
    own(7)
    for p in (4, 5, 6, 7):
        far(p)
    for way, d, k in late:
        z_copy(way, d, k).wait_send()


def write_kernel(keys_part, values_part, keys, values, sem):
    copies = []
    for h in range(2):
        for n in range(2):
            rows = pl.ds(96 * n, 96)
            copies.append(pltpu.make_async_copy(
                keys_part.at[h, rows], keys.at[0, h, rows], sem.at[len(copies)]
            ))
    for n in range(4):
        rows = pl.ds(2048 * n, 2048)
        copies.append(pltpu.make_async_copy(
            values_part.at[rows], values.at[rows], sem.at[len(copies)]
        ))
    for copy in copies:
        copy.start()
    for copy in copies:
        copy.wait()


def shards(latents, rotary_rows, latent_gain, key_up, value_up):
    shape = (lax.axis_size("span"), lax.axis_size("heads"), *latents.shape, rotary_rows.shape[2])
    if shape != (SPANS, RING, SPANS, COUNT, DEPTH, TURN) or key_up.shape != (DEPTH, 2, WIDTH) or (
        value_up.shape != (DEPTH, 2, WIDTH)
    ):
        return plain_shards(latents, rotary_rows, latent_gain, key_up, value_up)
    length = SPANS * RING * COUNT
    near = pl.BlockSpec(memory_space=pltpu.VMEM)
    far = pl.BlockSpec(memory_space=pltpu.HBM)
    args = (
        latents, rotary_rows, latent_gain[None],
        key_up.reshape(2 * DEPTH, WIDTH), value_up.reshape(2 * DEPTH, WIDTH),
    )
    parts = pl.pallas_call(
        exchange_kernel,
        out_shape=(
            pltpu.VMEM((2, WIDTH + TURN, length), BF16),
            pltpu.VMEM((2 * length, WIDTH), BF16),
        ),
        in_specs=[far] * 5,
        out_specs=[near] * 2,
        scratch_shapes=[
            pltpu.VMEM((RING, SPANS, TILES + 1, 16, 128), BF16),
            pltpu.VMEM((SPANS, TILES + 1, 16, 128), BF16),
            pltpu.VMEM((SPANS, COUNT, TURN), BF16),
            pltpu.VMEM((2, 2 * DEPTH, WIDTH), BF16),
            pltpu.VMEM((2 * WIDTH, DEPTH), BF16),
            pltpu.VMEM((DEPTH, 2 * WIDTH), BF16),
            pltpu.VMEM((1, DEPTH), F32),
            pltpu.VMEM((2, 64, 128), BF16),
            pltpu.VMEM((512, WIDTH), F32),
            pltpu.VMEM((256, DEPTH), BF16),
            pltpu.SemaphoreType.DMA((12,)),
            pltpu.SemaphoreType.DMA((SPANS,)),
            pltpu.SemaphoreType.DMA((SPANS,)),
            pltpu.SemaphoreType.DMA((8 * SPANS,)),
            pltpu.SemaphoreType.DMA((8 * SPANS,)),
        ],
        compiler_params=pltpu.CompilerParams(
            collective_id=0, has_side_effects=True, vmem_limit_bytes=40 * 1024 * 1024
        ),
    )(*(pltpu.with_memory_space_constraint(arg, pltpu.HBM) for arg in args))
    keys, values = pl.pallas_call(
        write_kernel,
        out_shape=(
            jax.ShapeDtypeStruct((1, 2, WIDTH + TURN, length), BF16),
            jax.ShapeDtypeStruct((2 * length, WIDTH), BF16),
        ),
        in_specs=[near] * 2,
        out_specs=[far] * 2,
        scratch_shapes=[pltpu.SemaphoreType.DMA((8,))],
        compiler_params=pltpu.CompilerParams(vmem_limit_bytes=16 * 1024 * 1024),
    )(*parts)
    return keys, values.reshape(1, length, 2, WIDTH)


def solution(mesh):
    return jax.shard_map(
        shards,
        mesh=mesh,
        in_specs=(
            P("trial", ("span", "heads"), None),
            P("trial", ("span", "heads"), None),
            P(),
            P("trial", "heads", None),
            P("trial", "heads", None),
        ),
        out_specs=(
            P(("trial", "span"), "heads", None, None),
            P(("trial", "span"), None, "heads", None),
        ),
        check_vma=False,
    )
```

```python
import functools

import jax
import jax.numpy as jnp
from jax import lax
from jax.experimental import pallas as pl
from jax.experimental.pallas import tpu as pltpu
from jax.sharding import PartitionSpec as P

MESH = pl.DeviceIdType.MESH
BF16, F32 = jnp.bfloat16, jnp.float32

SPANS, RING = 16, 8
COUNT, DEPTH = 32, 512
TURN, WIDTH = 64, 128
NEAR = 6
LAST = 7
TILES = 8


def widen_rows(rows, rotary, key_up, value_up):
    wide_keys = jnp.einsum(
        "btr,rhk->bthk", rows, key_up, preferred_element_type=jnp.float32
    ).astype(jnp.bfloat16)
    shared = jnp.broadcast_to(rotary[:, :, None], wide_keys.shape[:3] + rotary.shape[2:])
    wide_values = jnp.einsum(
        "btr,rhk->bthk", rows, value_up, preferred_element_type=jnp.float32
    ).astype(jnp.bfloat16)
    return (jnp.concatenate([wide_keys, shared], axis=-1), wide_values)


def unit_rows(vectors, row_gain):
    return (
        vectors * lax.rsqrt(jnp.mean(vectors * vectors, axis=-1, keepdims=True) + 1e-06) * row_gain
    )


def plain_shards(latents, rotary_rows, latent_gain, key_up, value_up):
    rows_ready = unit_rows(latents.astype(jnp.float32), latent_gain).astype(jnp.bfloat16)

    def move(block):
        block = lax.all_to_all(block, "span", split_axis=0, concat_axis=1, tiled=True)
        block = block.reshape(block.shape[0], lax.axis_size("span"), -1, block.shape[2])
        block = lax.all_gather(block, "heads", axis=2, tiled=True)
        return block.reshape(block.shape[0], -1, block.shape[3])

    cache_keys, cache_values = widen_rows(move(rows_ready), move(rotary_rows), key_up, value_up)
    return (jnp.transpose(cache_keys, (0, 2, 3, 1)), cache_values)


def source(me, k):
    j, flip = k // 2, k % 2
    away = ((j + 1) // 2) * (2 * (j % 2) - 1)
    core = (me % 2) * (1 - 2 * flip) + flip
    return ((me // 2 + away + SPANS // 2) % (SPANS // 2)) * 2 + core


def target(me, k):
    j, flip = k // 2, k % 2
    away = ((j + 1) // 2) * (2 * (j % 2) - 1)
    core = (me % 2) * (1 - 2 * flip) + flip
    return ((me // 2 - away + SPANS // 2) % (SPANS // 2)) * 2 + core


def y_unit(k):
    return (k,) if k < NEAR else (k // 2 * 2, k // 2 * 2 + 1)


def z_unit(d, k):
    return (k,) if (d == 1 and k < NEAR) or (d == 2 and k < 2) else (k // 2 * 2, k // 2 * 2 + 1)


def last_way(k):
    return k // 2 % 2


Y_SEMS, Z_SEMS = {}, {}
for place in range(SPANS):
    Y_SEMS[place] = len({y_unit(k) for k in range(1, place + 1)}) - 1
for way, hops, place in [(w, d, k) for w in range(2) for d in range(1, 5) for k in range(SPANS)]:
    if z_unit(hops, place)[0] == place and (hops < 4 or way == last_way(place)):
        Z_SEMS[way, hops, place] = len(Z_SEMS)


def expand_pair(tile, key_wide, value_wide, gain, pick, ready, flat, put_keys, put_values):
    for i in range(2):
        for zz in range(4):
            for half in range(2):
                raw = jnp.concatenate(
                    [tile(i, zz, half * 4 + c).astype(F32) for c in range(4)], axis=1
                )
                ready[pl.ds(i * 128 + zz * 32 + half * 16, 16), :] = (
                    unit_rows(raw, gain[...]).astype(BF16)
                )
    wide = lax.dot_general(
        key_wide[...], ready[...], (((1,), (1,)), ((), ())), preferred_element_type=F32
    ).astype(BF16)
    for i in range(2):
        turned = jnp.concatenate([tile(i, zz, TILES) for zz in range(4)], axis=0)
        halves = [
            lax.dot_general(
                turned, pick[half], (((0,), (0,)), ((), ())), preferred_element_type=F32
            )
            for half in range(2)
        ]
        shared = (halves[0][:TURN] + halves[1][TURN:]).astype(BF16)
        for h in range(2):
            put_keys(i, h, 0, wide[h * WIDTH:(h + 1) * WIDTH, i * 128:(i + 1) * 128])
            put_keys(i, h, WIDTH, shared)
    wide = jnp.dot(ready[...], value_wide[...], preferred_element_type=F32)
    for h in range(2):
        flat[pl.ds(h, 256, stride=2), :] = wide[:, h * WIDTH:(h + 1) * WIDTH]
    for i in range(2):
        put_values(i, flat[pl.ds(i * 256, 256), :].astype(BF16))


def exchange_kernel(
    lat, rot, far_gain, key_up, value_up, keys, values, late, key_wide, value_wide, gain, pick,
    buf, stage, rot_raw, raw_w, flat,
    ready, load_sem, y_send, y_recv, z_send, z_recv, round_sem,
):
    me, z = lax.axis_index("span"), lax.axis_index("heads")
    ahead, behind = lax.rem(z + 1, RING), lax.rem(z + RING - 1, RING)

    sibling = target(me, 1)

    rot_load = pltpu.make_async_copy(rot, rot_raw, load_sem.at[0])
    rot_load.start()
    for t in range(TILES):
        rows = pl.ds(16 * (t // 4), 16)
        columns = pl.ds(128 * (t % 4), 128)
        pltpu.make_async_copy(
            lat.at[:, rows, columns], stage.at[:, t], load_sem.at[1]
        ).start()
    gain_load = pltpu.make_async_copy(far_gain, gain, load_sem.at[2])
    gain_load.start()
    for w, weight in enumerate((key_up, value_up)):
        pltpu.make_async_copy(weight, raw_w.at[w], load_sem.at[3]).start()

    barrier = pltpu.get_barrier_semaphore()
    greeted = [{"heads": near} for near in (ahead, behind)] + [{"span": target(me, k)} for k in range(1, NEAR)]
    greeted += [{"span": sibling, "heads": near} for near in (ahead, behind)]
    for device in greeted:
        pl.semaphore_signal(barrier, inc=1, device_id=device, device_id_type=MESH)

    rot_load.wait()
    for s in range(SPANS):
        part = rot_raw[s].astype(F32)
        stage[s, TILES] = jnp.concatenate([part[:16], part[16:]], axis=1).astype(BF16)

    all_rows = stage.at[:, pl.ds(0, TILES)]
    pltpu.make_async_copy(all_rows, all_rows, load_sem.at[1]).wait()
    pl.semaphore_wait(barrier, len(greeted))
    for near in (ahead, behind):
        pl.semaphore_signal(round_sem, inc=1, device_id={"heads": near}, device_id_type=MESH)

    def z_copy(way, d, ks):
        if way == 0:
            here, there, to = (RING + 1 - d) % RING, RING - d, ahead
        else:
            here, there, to = d - 1, d, behind
        places = pl.ds(ks[0], len(ks))
        src, device = buf.at[here, places], {"heads": to}
        if d == 1 and ks == (0,):
            src = stage.at[pl.ds(me, 1)]
        elif d == 1 and ks[0] < NEAR:
            to_span = target(me, ks[0])
            src, device = stage.at[pl.ds(to_span, 1)], {"span": to_span, "heads": to}
        return pltpu.make_async_remote_copy(
            src_ref=src, dst_ref=buf.at[there, places],
            send_sem=z_send.at[0], recv_sem=z_recv.at[Z_SEMS[way, d, ks[0]]],
            device_id=device, device_id_type=MESH,
        )

    def y_copy(k):
        to = target(me, k)
        return pltpu.make_async_remote_copy(
            src_ref=stage.at[pl.ds(to, 1)], dst_ref=buf.at[0, pl.ds(k, 1)],
            send_sem=y_send.at[0], recv_sem=y_recv.at[Y_SEMS[k]],
            device_id={"span": to}, device_id_type=MESH,
        )

    heard = set()

    def need(way, d, k):
        if d == 0:
            ks = y_unit(k)
            if ks != (0,) and (0, ks) not in heard:
                heard.add((0, ks))
                places = buf.at[0, pl.ds(ks[0], len(ks))]
                pltpu.make_async_remote_copy(
                    src_ref=places, dst_ref=places, send_sem=y_send.at[0],
                    recv_sem=y_recv.at[Y_SEMS[ks[0]]],
                    device_id={"span": sibling}, device_id_type=MESH,
                ).wait_recv()
            return
        ks = z_unit(d, k)
        if (way, d, ks) not in heard:
            heard.add((way, d, ks))
            z_copy(way, d, ks).wait_recv()

    def forward(d, ks):
        for unit in dict.fromkeys(z_unit(d, k) for k in ks):
            for way in (0, 1):
                if d > 1 or unit[0] >= NEAR:
                    for k in unit:
                        need(way, d - 1, k)
                if d < 4 or way == last_way(unit[0]):
                    z_copy(way, d, unit).start()

    def spread(ks):
        for k in ks:
            y_copy(k).start()

    forward(1, [0, 1])
    spread(range(1, NEAR))
    buf[0, 0] = stage[me]

    gain_load.wait()
    pltpu.make_async_copy(raw_w, raw_w, load_sem.at[3]).wait()
    for w, put in ((0, key_wide), (1, value_wide)):
        @pl.loop(0, 4)
        def _(n):
            r = pl.multiple_of(n * 256, 256)
            flat[pl.ds(0, 256), :] = raw_w[w, pl.ds(r, 256), :].astype(F32)
            at = pl.multiple_of(n * 128, 128)
            for h in range(2):
                block = flat[pl.ds(h, 128, stride=2), :]
                if w == 0:
                    key_wide[h * WIDTH:(h + 1) * WIDTH, pl.ds(at, 128)] = block.T.astype(BF16)
                else:
                    value_wide[pl.ds(at, 128), h * WIDTH:(h + 1) * WIDTH] = block.astype(BF16)
    row = lax.broadcasted_iota(jnp.int32, (64, 128), 0)
    column = lax.broadcasted_iota(jnp.int32, (64, 128), 1)
    for half in range(2):
        place = (row // 16) * 32 + half * 16 + row % 16
        pick[half] = jnp.where(place == column, 1.0, 0.0).astype(BF16)

    def expand(p, other):
        group = z // 4 if not other else 1 - z // 4
        pair = (2 * p, 2 * p + 1)
        for k in pair:
            need(0, 0, k)
            for way in (0, 1):
                need(way, 3, k)
            if other:
                need(last_way(k), 4, k)
        rels = [lax.rem(group * 4 + zz + RING - z, RING) for zz in range(4)]
        if other and p == LAST:
            for i, k in enumerate(pair):
                for zz in range(4):
                    late[i, zz] = buf[rels[zz], k]
            return
        starts = [pl.multiple_of(source(me, k) * 256 + group * 128, 128) for k in pair]

        def put_keys(i, h, first, block):
            keys[h, first:first + block.shape[0], pl.ds(starts[i], 128)] = block

        def put_values(i, block):
            values[pl.ds(pl.multiple_of(starts[i] * 2, 256), 256), :] = block

        expand_pair(
            lambda i, zz, t: buf[rels[zz], pair[i], t],
            key_wide, value_wide, gain, pick, ready, flat, put_keys, put_values,
        )

    def hop(d, *pairs):
        for p in pairs:
            forward(d, [2 * p, 2 * p + 1])

    own, far = functools.partial(expand, other=False), functools.partial(expand, other=True)

    pl.semaphore_wait(round_sem, 2)
    forward(1, range(2, NEAR))
    forward(2, [0])
    for k in range(2, NEAR):
        need(0, 0, k)
    spread(range(NEAR, 10))
    forward(2, [1])
    hop(2, 1, 2)
    hop(1, 3, 4)
    spread(range(10, 16))
    hop(3, 0)
    hop(2, 3, 4)
    hop(1, 5, 6)
    hop(3, 1)
    hop(2, 5)
    own(0)
    hop(2, 6)
    hop(1, 7)
    hop(3, 2)
    hop(3, 3)
    own(1)
    hop(2, 7)
    hop(3, 4)
    own(2)
    hop(4, 0, 1)
    own(3)
    hop(3, 5)
    hop(3, 6)
    far(0)
    hop(3, 7)
    own(4)
    hop(4, 2, 3)
    far(1)
    own(5)
    hop(4, 4, 5)
    own(6)
    hop(4, 6, 7)
    own(7)
    for p in range(2, 8):
        far(p)
    for held, sem in ((buf.at[pl.ds(0, RING - 1)], z_send), (stage.at[pl.ds(0, SPANS - 1)], y_send)):
        pltpu.make_async_remote_copy(
            src_ref=held, dst_ref=held, send_sem=sem.at[0], recv_sem=y_recv.at[0],
            device_id={"span": sibling}, device_id_type=MESH,
        ).wait_send()


def write_kernel(
    keys_part, values_part, late, key_wide, value_wide, gain, pick, keys, values,
    ready, flat, keys_late, values_late, sem,
):
    me, z = lax.axis_index("span"), lax.axis_index("heads")
    near, away = z // 4, 1 - z // 4
    for k in range(SPANS):
        first, size = source(me, k) * 256, 256
        if k // 2 == LAST:
            first, size = first + near * 128, 128
        columns = pl.ds(pl.multiple_of(first, 128), size)
        rows = pl.ds(pl.multiple_of(first * 2, 256), size * 2)
        pltpu.make_async_copy(keys_part.at[:, :, columns], keys.at[0, :, :, columns], sem.at[0]).start()
        pltpu.make_async_copy(values_part.at[rows], values.at[rows], sem.at[1]).start()

    def put_keys(i, h, first, block):
        keys_late[i, h, first:first + block.shape[0], :] = block

    def put_values(i, block):
        values_late[i] = block

    expand_pair(
        lambda i, zz, t: late[i, zz, t],
        key_wide, value_wide, gain, pick, ready, flat, put_keys, put_values,
    )
    for i in range(2):
        first = source(me, 2 * LAST + i) * 256 + away * 128
        columns = pl.ds(pl.multiple_of(first, 128), 128)
        rows = pl.ds(pl.multiple_of(first * 2, 256), 256)
        pltpu.make_async_copy(keys_late.at[i], keys.at[0, :, :, columns], sem.at[2]).start()
        pltpu.make_async_copy(values_late.at[i], values.at[rows], sem.at[3]).start()
    length = keys_part.shape[2]
    early = (keys_part.at[:, :, pl.ds(0, length - 256)], values_part.at[pl.ds(0, 2 * length - 512)])
    for n, held in enumerate((*early, keys_late, values_late)):
        pltpu.make_async_copy(held, held, sem.at[n]).wait()


def shards(latents, rotary_rows, latent_gain, key_up, value_up):
    shape = (lax.axis_size("span"), lax.axis_size("heads"), *latents.shape, rotary_rows.shape[2])
    if shape != (SPANS, RING, SPANS, COUNT, DEPTH, TURN) or key_up.shape != (DEPTH, 2, WIDTH) or (
        value_up.shape != (DEPTH, 2, WIDTH)
    ):
        return plain_shards(latents, rotary_rows, latent_gain, key_up, value_up)
    length = SPANS * RING * COUNT
    near = pl.BlockSpec(memory_space=pltpu.VMEM)
    far = pl.BlockSpec(memory_space=pltpu.HBM)
    args = (
        latents, rotary_rows, latent_gain[None],
        key_up.reshape(2 * DEPTH, WIDTH), value_up.reshape(2 * DEPTH, WIDTH),
    )
    parts = pl.pallas_call(
        exchange_kernel,
        out_shape=(
            pltpu.VMEM((2, WIDTH + TURN, length), BF16),
            pltpu.VMEM((2 * length, WIDTH), BF16),
            pltpu.VMEM((2, 4, TILES + 1, 16, 128), BF16),
            pltpu.VMEM((2 * WIDTH, DEPTH), BF16),
            pltpu.VMEM((DEPTH, 2 * WIDTH), BF16),
            pltpu.VMEM((1, DEPTH), F32),
            pltpu.VMEM((2, 64, 128), BF16),
        ),
        in_specs=[far] * 5,
        out_specs=[near] * 7,
        scratch_shapes=[
            pltpu.VMEM((RING, SPANS, TILES + 1, 16, 128), BF16),
            pltpu.VMEM((SPANS, TILES + 1, 16, 128), BF16),
            pltpu.VMEM((SPANS, COUNT, TURN), BF16),
            pltpu.VMEM((2, 2 * DEPTH, WIDTH), BF16),
            pltpu.VMEM((512, WIDTH), F32),
            pltpu.VMEM((256, DEPTH), BF16),
            pltpu.SemaphoreType.DMA((4,)),
            pltpu.SemaphoreType.DMA((1,)),
            pltpu.SemaphoreType.DMA((Y_SEMS[SPANS - 1] + 1,)),
            pltpu.SemaphoreType.DMA((1,)),
            pltpu.SemaphoreType.DMA((len(Z_SEMS),)),
            pltpu.SemaphoreType.REGULAR,
        ],
        compiler_params=pltpu.CompilerParams(
            collective_id=0, has_side_effects=True, vmem_limit_bytes=40 * 1024 * 1024
        ),
    )(*(pltpu.with_memory_space_constraint(arg, pltpu.HBM) for arg in args))
    keys, values = pl.pallas_call(
        write_kernel,
        out_shape=(
            jax.ShapeDtypeStruct((1, 2, WIDTH + TURN, length), BF16),
            jax.ShapeDtypeStruct((2 * length, WIDTH), BF16),
        ),
        in_specs=[near] * 7,
        out_specs=[far] * 2,
        scratch_shapes=[
            pltpu.VMEM((256, DEPTH), BF16),
            pltpu.VMEM((512, WIDTH), F32),
            pltpu.VMEM((2, 2, WIDTH + TURN, 128), BF16),
            pltpu.VMEM((2, 256, WIDTH), BF16),
            pltpu.SemaphoreType.DMA((4,)),
        ],
        compiler_params=pltpu.CompilerParams(vmem_limit_bytes=16 * 1024 * 1024),
    )(*parts)
    return keys, values.reshape(1, length, 2, WIDTH)


def solution(mesh):
    return jax.shard_map(
        shards,
        mesh=mesh,
        in_specs=(
            P("trial", ("span", "heads"), None),
            P("trial", ("span", "heads"), None),
            P(),
            P("trial", "heads", None),
            P("trial", "heads", None),
        ),
        out_specs=(
            P(("trial", "span"), "heads", None, None),
            P(("trial", "span"), None, "heads", None),
        ),
        check_vma=False,
    )
```

```python
import functools

import jax
import jax.numpy as jnp
from jax import lax
from jax.experimental import pallas as pl
from jax.experimental.pallas import tpu as pltpu
from jax.sharding import PartitionSpec as P

MESH = pl.DeviceIdType.MESH
BF16, F32 = jnp.bfloat16, jnp.float32

SPANS, RING = 16, 8
COUNT, DEPTH = 32, 512
TURN, WIDTH = 64, 128
NEAR = 6
LAST = 7
TILES = 8


def widen_rows(rows, rotary, key_up, value_up):
    wide_keys = jnp.einsum(
        "btr,rhk->bthk", rows, key_up, preferred_element_type=jnp.float32
    ).astype(jnp.bfloat16)
    shared = jnp.broadcast_to(rotary[:, :, None], wide_keys.shape[:3] + rotary.shape[2:])
    wide_values = jnp.einsum(
        "btr,rhk->bthk", rows, value_up, preferred_element_type=jnp.float32
    ).astype(jnp.bfloat16)
    return (jnp.concatenate([wide_keys, shared], axis=-1), wide_values)


def unit_rows(vectors, row_gain):
    return (
        vectors * lax.rsqrt(jnp.mean(vectors * vectors, axis=-1, keepdims=True) + 1e-06) * row_gain
    )


def plain_shards(latents, rotary_rows, latent_gain, key_up, value_up):
    rows_ready = unit_rows(latents.astype(jnp.float32), latent_gain).astype(jnp.bfloat16)

    def move(block):
        block = lax.all_to_all(block, "span", split_axis=0, concat_axis=1, tiled=True)
        block = block.reshape(block.shape[0], lax.axis_size("span"), -1, block.shape[2])
        block = lax.all_gather(block, "heads", axis=2, tiled=True)
        return block.reshape(block.shape[0], -1, block.shape[3])

    cache_keys, cache_values = widen_rows(move(rows_ready), move(rotary_rows), key_up, value_up)
    return (jnp.transpose(cache_keys, (0, 2, 3, 1)), cache_values)


def source(me, k):
    j, flip = k // 2, k % 2
    away = ((j + 1) // 2) * (2 * (j % 2) - 1)
    core = (me % 2) * (1 - 2 * flip) + flip
    return ((me // 2 + away + SPANS // 2) % (SPANS // 2)) * 2 + core


def target(me, k):
    j, flip = k // 2, k % 2
    away = ((j + 1) // 2) * (2 * (j % 2) - 1)
    core = (me % 2) * (1 - 2 * flip) + flip
    return ((me // 2 - away + SPANS // 2) % (SPANS // 2)) * 2 + core


def y_unit(k):
    return (k,) if k < NEAR else (k // 2 * 2, k // 2 * 2 + 1)


def z_unit(d, k):
    alone = (d == 1 and k < NEAR) or (d == 2 and k < 2) or d == 4
    return (k,) if alone else (k // 2 * 2, k // 2 * 2 + 1)


def last_way(k):
    return k % 2


Y_SEMS, Z_SEMS = {}, {}
for place in range(SPANS):
    Y_SEMS[place] = len({y_unit(k) for k in range(1, place + 1)}) - 1
for way, hops, place in [(w, d, k) for w in range(2) for d in range(1, 5) for k in range(SPANS)]:
    if z_unit(hops, place)[0] == place and (hops < 4 or way == last_way(place)):
        Z_SEMS[way, hops, place] = len(Z_SEMS)


def expand_pair(tile, key_wide, value_wide, gain, pick, ready, flat, put_keys, put_values):
    for i in range(2):
        for zz in range(4):
            for half in range(2):
                raw = jnp.concatenate(
                    [tile(i, zz, half * 4 + c).astype(F32) for c in range(4)], axis=1
                )
                ready[pl.ds(i * 128 + zz * 32 + half * 16, 16), :] = (
                    unit_rows(raw, gain[...]).astype(BF16)
                )
    wide = lax.dot_general(
        key_wide[...], ready[...], (((1,), (1,)), ((), ())), preferred_element_type=F32
    ).astype(BF16)
    for i in range(2):
        turned = jnp.concatenate([tile(i, zz, TILES) for zz in range(4)], axis=0)
        halves = [
            lax.dot_general(
                turned, pick[half], (((0,), (0,)), ((), ())), preferred_element_type=F32
            )
            for half in range(2)
        ]
        shared = (halves[0][:TURN] + halves[1][TURN:]).astype(BF16)
        for h in range(2):
            put_keys(i, h, 0, wide[h * WIDTH:(h + 1) * WIDTH, i * 128:(i + 1) * 128])
            put_keys(i, h, WIDTH, shared)
    wide = jnp.dot(ready[...], value_wide[...], preferred_element_type=F32)
    for h in range(2):
        flat[pl.ds(h, 256, stride=2), :] = wide[:, h * WIDTH:(h + 1) * WIDTH]
    for i in range(2):
        put_values(i, flat[pl.ds(i * 256, 256), :].astype(BF16))


def exchange_kernel(
    lat, rot, far_gain, key_up, value_up, keys, values, late, key_wide, value_wide, gain, pick,
    buf, stage, rot_raw, raw_w, flat,
    ready, load_sem, y_send, y_recv, z_send, z_recv, round_sem,
):
    me, z = lax.axis_index("span"), lax.axis_index("heads")
    ahead, behind = lax.rem(z + 1, RING), lax.rem(z + RING - 1, RING)

    sibling = target(me, 1)

    rot_load = pltpu.make_async_copy(rot, rot_raw, load_sem.at[0])
    rot_load.start()
    for t in range(TILES):
        rows = pl.ds(16 * (t // 4), 16)
        columns = pl.ds(128 * (t % 4), 128)
        pltpu.make_async_copy(
            lat.at[:, rows, columns], stage.at[:, t], load_sem.at[1]
        ).start()
    gain_load = pltpu.make_async_copy(far_gain, gain, load_sem.at[2])
    gain_load.start()
    for w, weight in enumerate((key_up, value_up)):
        pltpu.make_async_copy(weight, raw_w.at[w], load_sem.at[3]).start()

    barrier = pltpu.get_barrier_semaphore()
    greeted = [{"heads": near} for near in (ahead, behind)] + [{"span": target(me, k)} for k in range(1, NEAR)]
    greeted += [{"span": sibling, "heads": near} for near in (ahead, behind)]
    for device in greeted:
        pl.semaphore_signal(barrier, inc=1, device_id=device, device_id_type=MESH)

    rot_load.wait()
    for s in range(SPANS):
        part = rot_raw[s].astype(F32)
        stage[s, TILES] = jnp.concatenate([part[:16], part[16:]], axis=1).astype(BF16)

    all_rows = stage.at[:, pl.ds(0, TILES)]
    pltpu.make_async_copy(all_rows, all_rows, load_sem.at[1]).wait()
    pl.semaphore_wait(barrier, len(greeted))
    for near in (ahead, behind):
        pl.semaphore_signal(round_sem, inc=1, device_id={"heads": near}, device_id_type=MESH)

    def z_copy(way, d, ks):
        if way == 0:
            here, there, to = (RING + 1 - d) % RING, RING - d, ahead
        else:
            here, there, to = d - 1, d, behind
        places = pl.ds(ks[0], len(ks))
        src, device = buf.at[here, places], {"heads": to}
        if d == 1 and ks == (0,):
            src = stage.at[pl.ds(me, 1)]
        elif d == 1 and ks[0] < NEAR:
            to_span = target(me, ks[0])
            src, device = stage.at[pl.ds(to_span, 1)], {"span": to_span, "heads": to}
        return pltpu.make_async_remote_copy(
            src_ref=src, dst_ref=buf.at[there, places],
            send_sem=z_send.at[0], recv_sem=z_recv.at[Z_SEMS[way, d, ks[0]]],
            device_id=device, device_id_type=MESH,
        )

    def y_copy(k):
        to = target(me, k)
        return pltpu.make_async_remote_copy(
            src_ref=stage.at[pl.ds(to, 1)], dst_ref=buf.at[0, pl.ds(k, 1)],
            send_sem=y_send.at[0], recv_sem=y_recv.at[Y_SEMS[k]],
            device_id={"span": to}, device_id_type=MESH,
        )

    heard = set()

    def need(way, d, k):
        if d == 0:
            ks = y_unit(k)
            if ks != (0,) and (0, ks) not in heard:
                heard.add((0, ks))
                places = buf.at[0, pl.ds(ks[0], len(ks))]
                pltpu.make_async_remote_copy(
                    src_ref=places, dst_ref=places, send_sem=y_send.at[0],
                    recv_sem=y_recv.at[Y_SEMS[ks[0]]],
                    device_id={"span": sibling}, device_id_type=MESH,
                ).wait_recv()
            return
        ks = z_unit(d, k)
        if (way, d, ks) not in heard:
            heard.add((way, d, ks))
            z_copy(way, d, ks).wait_recv()

    def forward(d, ks):
        for unit in dict.fromkeys(z_unit(d, k) for k in ks):
            for way in (0, 1):
                if d > 1 or unit[0] >= NEAR:
                    for k in unit:
                        need(way, d - 1, k)
                if d < 4 or way == last_way(unit[0]):
                    z_copy(way, d, unit).start()

    def spread(ks):
        for k in ks:
            y_copy(k).start()

    forward(1, [0, 1])
    spread(range(1, NEAR))
    buf[0, 0] = stage[me]

    gain_load.wait()
    pltpu.make_async_copy(raw_w, raw_w, load_sem.at[3]).wait()
    for w, put in ((0, key_wide), (1, value_wide)):
        @pl.loop(0, 4)
        def _(n):
            r = pl.multiple_of(n * 256, 256)
            flat[pl.ds(0, 256), :] = raw_w[w, pl.ds(r, 256), :].astype(F32)
            at = pl.multiple_of(n * 128, 128)
            for h in range(2):
                block = flat[pl.ds(h, 128, stride=2), :]
                if w == 0:
                    key_wide[h * WIDTH:(h + 1) * WIDTH, pl.ds(at, 128)] = block.T.astype(BF16)
                else:
                    value_wide[pl.ds(at, 128), h * WIDTH:(h + 1) * WIDTH] = block.astype(BF16)
    row = lax.broadcasted_iota(jnp.int32, (64, 128), 0)
    column = lax.broadcasted_iota(jnp.int32, (64, 128), 1)
    for half in range(2):
        place = (row // 16) * 32 + half * 16 + row % 16
        pick[half] = jnp.where(place == column, 1.0, 0.0).astype(BF16)

    def expand(p, other):
        group = z // 4 if not other else 1 - z // 4
        pair = (2 * p, 2 * p + 1)
        for k in pair:
            need(0, 0, k)
            for way in (0, 1):
                need(way, 3, k)
            if other:
                need(last_way(k), 4, k)
        rels = [lax.rem(group * 4 + zz + RING - z, RING) for zz in range(4)]
        if other and p == LAST:
            for i, k in enumerate(pair):
                for zz in range(4):
                    late[i, zz] = buf[rels[zz], k]
            return
        starts = [pl.multiple_of(source(me, k) * 256 + group * 128, 128) for k in pair]

        def put_keys(i, h, first, block):
            keys[h, first:first + block.shape[0], pl.ds(starts[i], 128)] = block

        def put_values(i, block):
            values[pl.ds(pl.multiple_of(starts[i] * 2, 256), 256), :] = block

        expand_pair(
            lambda i, zz, t: buf[rels[zz], pair[i], t],
            key_wide, value_wide, gain, pick, ready, flat, put_keys, put_values,
        )

    def hop(d, *pairs):
        for p in pairs:
            forward(d, [2 * p, 2 * p + 1])

    own, far = functools.partial(expand, other=False), functools.partial(expand, other=True)

    pl.semaphore_wait(round_sem, 2)
    forward(1, range(2, NEAR))
    forward(2, [0])
    for k in range(2, NEAR):
        need(0, 0, k)
    spread(range(NEAR, 10))
    forward(2, [1])
    hop(2, 1, 2)
    hop(1, 3, 4)
    spread(range(10, 16))
    hop(3, 0)
    hop(2, 3, 4)
    hop(3, 1)
    hop(1, 5, 6)
    hop(2, 5)
    own(0)
    hop(2, 6)
    hop(1, 7)
    hop(3, 2)
    hop(3, 3)
    own(1)
    hop(2, 7)
    hop(3, 4)
    hop(4, 0, 1)
    own(2)
    hop(3, 5)
    hop(3, 6)
    own(3)
    hop(3, 7)
    hop(4, 2, 3)
    own(4)
    far(0)
    far(1)
    hop(4, 4, 5)
    own(5)
    hop(4, 6, 7)
    own(6)
    own(7)
    for p in range(2, 8):
        far(p)
    for held, sem in ((buf.at[pl.ds(0, RING - 1)], z_send), (stage.at[pl.ds(0, SPANS - 1)], y_send)):
        pltpu.make_async_remote_copy(
            src_ref=held, dst_ref=held, send_sem=sem.at[0], recv_sem=y_recv.at[0],
            device_id={"span": sibling}, device_id_type=MESH,
        ).wait_send()


def write_kernel(
    keys_part, values_part, late, key_wide, value_wide, gain, pick, keys, values,
    ready, flat, keys_late, values_late, sem,
):
    me, z = lax.axis_index("span"), lax.axis_index("heads")
    near, away = z // 4, 1 - z // 4
    for k in range(SPANS):
        first, size = source(me, k) * 256, 256
        if k // 2 == LAST:
            first, size = first + near * 128, 128
        columns = pl.ds(pl.multiple_of(first, 128), size)
        rows = pl.ds(pl.multiple_of(first * 2, 256), size * 2)
        pltpu.make_async_copy(keys_part.at[:, :, columns], keys.at[0, :, :, columns], sem.at[0]).start()
        pltpu.make_async_copy(values_part.at[rows], values.at[rows], sem.at[1]).start()

    def put_keys(i, h, first, block):
        keys_late[i, h, first:first + block.shape[0], :] = block

    def put_values(i, block):
        values_late[i] = block

    expand_pair(
        lambda i, zz, t: late[i, zz, t],
        key_wide, value_wide, gain, pick, ready, flat, put_keys, put_values,
    )
    for i in range(2):
        first = source(me, 2 * LAST + i) * 256 + away * 128
        columns = pl.ds(pl.multiple_of(first, 128), 128)
        rows = pl.ds(pl.multiple_of(first * 2, 256), 256)
        pltpu.make_async_copy(keys_late.at[i], keys.at[0, :, :, columns], sem.at[2]).start()
        pltpu.make_async_copy(values_late.at[i], values.at[rows], sem.at[3]).start()
    length = keys_part.shape[2]
    early = (keys_part.at[:, :, pl.ds(0, length - 256)], values_part.at[pl.ds(0, 2 * length - 512)])
    for n, held in enumerate((*early, keys_late, values_late)):
        pltpu.make_async_copy(held, held, sem.at[n]).wait()


def shards(latents, rotary_rows, latent_gain, key_up, value_up):
    shape = (lax.axis_size("span"), lax.axis_size("heads"), *latents.shape, rotary_rows.shape[2])
    if shape != (SPANS, RING, SPANS, COUNT, DEPTH, TURN) or key_up.shape != (DEPTH, 2, WIDTH) or (
        value_up.shape != (DEPTH, 2, WIDTH)
    ):
        return plain_shards(latents, rotary_rows, latent_gain, key_up, value_up)
    length = SPANS * RING * COUNT
    near = pl.BlockSpec(memory_space=pltpu.VMEM)
    far = pl.BlockSpec(memory_space=pltpu.HBM)
    args = (
        latents, rotary_rows, latent_gain[None],
        key_up.reshape(2 * DEPTH, WIDTH), value_up.reshape(2 * DEPTH, WIDTH),
    )
    parts = pl.pallas_call(
        exchange_kernel,
        out_shape=(
            pltpu.VMEM((2, WIDTH + TURN, length), BF16),
            pltpu.VMEM((2 * length, WIDTH), BF16),
            pltpu.VMEM((2, 4, TILES + 1, 16, 128), BF16),
            pltpu.VMEM((2 * WIDTH, DEPTH), BF16),
            pltpu.VMEM((DEPTH, 2 * WIDTH), BF16),
            pltpu.VMEM((1, DEPTH), F32),
            pltpu.VMEM((2, 64, 128), BF16),
        ),
        in_specs=[far] * 5,
        out_specs=[near] * 7,
        scratch_shapes=[
            pltpu.VMEM((RING, SPANS, TILES + 1, 16, 128), BF16),
            pltpu.VMEM((SPANS, TILES + 1, 16, 128), BF16),
            pltpu.VMEM((SPANS, COUNT, TURN), BF16),
            pltpu.VMEM((2, 2 * DEPTH, WIDTH), BF16),
            pltpu.VMEM((512, WIDTH), F32),
            pltpu.VMEM((256, DEPTH), BF16),
            pltpu.SemaphoreType.DMA((4,)),
            pltpu.SemaphoreType.DMA((1,)),
            pltpu.SemaphoreType.DMA((Y_SEMS[SPANS - 1] + 1,)),
            pltpu.SemaphoreType.DMA((1,)),
            pltpu.SemaphoreType.DMA((len(Z_SEMS),)),
            pltpu.SemaphoreType.REGULAR,
        ],
        compiler_params=pltpu.CompilerParams(
            collective_id=0, has_side_effects=True, vmem_limit_bytes=40 * 1024 * 1024
        ),
    )(*(pltpu.with_memory_space_constraint(arg, pltpu.HBM) for arg in args))
    keys, values = pl.pallas_call(
        write_kernel,
        out_shape=(
            jax.ShapeDtypeStruct((1, 2, WIDTH + TURN, length), BF16),
            jax.ShapeDtypeStruct((2 * length, WIDTH), BF16),
        ),
        in_specs=[near] * 7,
        out_specs=[far] * 2,
        scratch_shapes=[
            pltpu.VMEM((256, DEPTH), BF16),
            pltpu.VMEM((512, WIDTH), F32),
            pltpu.VMEM((2, 2, WIDTH + TURN, 128), BF16),
            pltpu.VMEM((2, 256, WIDTH), BF16),
            pltpu.SemaphoreType.DMA((4,)),
        ],
        compiler_params=pltpu.CompilerParams(vmem_limit_bytes=16 * 1024 * 1024),
    )(*parts)
    return keys, values.reshape(1, length, 2, WIDTH)


def solution(mesh):
    return jax.shard_map(
        shards,
        mesh=mesh,
        in_specs=(
            P("trial", ("span", "heads"), None),
            P("trial", ("span", "heads"), None),
            P(),
            P("trial", "heads", None),
            P("trial", "heads", None),
        ),
        out_specs=(
            P(("trial", "span"), "heads", None, None),
            P(("trial", "span"), None, "heads", None),
        ),
        check_vma=False,
    )
```

```python
import functools

import jax
import jax.numpy as jnp
from jax import lax
from jax.experimental import pallas as pl
from jax.experimental.pallas import tpu as pltpu
from jax.sharding import PartitionSpec as P

MESH = pl.DeviceIdType.MESH
BF16, F32 = jnp.bfloat16, jnp.float32

SPANS, RING = 16, 8
COUNT, DEPTH = 32, 512
TURN, WIDTH = 64, 128
NEAR = 6
LAST = 7
TILES = 8


def widen_rows(rows, rotary, key_up, value_up):
    wide_keys = jnp.einsum(
        "btr,rhk->bthk", rows, key_up, preferred_element_type=jnp.float32
    ).astype(jnp.bfloat16)
    shared = jnp.broadcast_to(rotary[:, :, None], wide_keys.shape[:3] + rotary.shape[2:])
    wide_values = jnp.einsum(
        "btr,rhk->bthk", rows, value_up, preferred_element_type=jnp.float32
    ).astype(jnp.bfloat16)
    return (jnp.concatenate([wide_keys, shared], axis=-1), wide_values)


def unit_rows(vectors, row_gain):
    return (
        vectors * lax.rsqrt(jnp.mean(vectors * vectors, axis=-1, keepdims=True) + 1e-06) * row_gain
    )


def plain_shards(latents, rotary_rows, latent_gain, key_up, value_up):
    rows_ready = unit_rows(latents.astype(jnp.float32), latent_gain).astype(jnp.bfloat16)

    def move(block):
        block = lax.all_to_all(block, "span", split_axis=0, concat_axis=1, tiled=True)
        block = block.reshape(block.shape[0], lax.axis_size("span"), -1, block.shape[2])
        block = lax.all_gather(block, "heads", axis=2, tiled=True)
        return block.reshape(block.shape[0], -1, block.shape[3])

    cache_keys, cache_values = widen_rows(move(rows_ready), move(rotary_rows), key_up, value_up)
    return (jnp.transpose(cache_keys, (0, 2, 3, 1)), cache_values)


def source(me, k):
    j, flip = k // 2, k % 2
    away = ((j + 1) // 2) * (2 * (j % 2) - 1)
    core = (me % 2) * (1 - 2 * flip) + flip
    return ((me // 2 + away + SPANS // 2) % (SPANS // 2)) * 2 + core


def target(me, k):
    j, flip = k // 2, k % 2
    away = ((j + 1) // 2) * (2 * (j % 2) - 1)
    core = (me % 2) * (1 - 2 * flip) + flip
    return ((me // 2 - away + SPANS // 2) % (SPANS // 2)) * 2 + core


def y_unit(k):
    return (k,) if k < NEAR else (k // 2 * 2, k // 2 * 2 + 1)


def z_unit(d, k):
    alone = (d == 1 and k < NEAR) or (d == 2 and k < 2) or d == 4
    return (k,) if alone else (k // 2 * 2, k // 2 * 2 + 1)


def wait_unit(d, k):
    return z_unit(d, k) if d < 3 and k < 2 else (k // 2 * 2, k // 2 * 2 + 1)


def last_way(k):
    return k % 2


Y_SEMS, Z_SEMS = {}, {}
for place in range(SPANS):
    Y_SEMS[place] = len({y_unit(k) for k in range(1, place + 1)}) - 1
for way, hops, place in [(w, d, k) for w in range(2) for d in range(1, 5) for k in range(SPANS)]:
    first = (0 if hops == 4 else way, hops, wait_unit(hops, place)[0])
    Z_SEMS[way, hops, place] = Z_SEMS.setdefault(first, len(set(Z_SEMS.values())))


def expand_pair(tile, key_wide, value_wide, gain, pick, ready, flat, put_keys, put_values):
    for i in range(2):
        for zz in range(4):
            for half in range(2):
                raw = jnp.concatenate(
                    [tile(i, zz, half * 4 + c).astype(F32) for c in range(4)], axis=1
                )
                ready[pl.ds(i * 128 + zz * 32 + half * 16, 16), :] = (
                    unit_rows(raw, gain[...]).astype(BF16)
                )
    wide = lax.dot_general(
        key_wide[...], ready[...], (((1,), (1,)), ((), ())), preferred_element_type=F32
    ).astype(BF16)
    for i in range(2):
        turned = jnp.concatenate([tile(i, zz, TILES) for zz in range(4)], axis=0)
        halves = [
            lax.dot_general(
                turned, pick[half], (((0,), (0,)), ((), ())), preferred_element_type=F32
            )
            for half in range(2)
        ]
        shared = (halves[0][:TURN] + halves[1][TURN:]).astype(BF16)
        for h in range(2):
            put_keys(i, h, 0, wide[h * WIDTH:(h + 1) * WIDTH, i * 128:(i + 1) * 128])
            put_keys(i, h, WIDTH, shared)
    wide = jnp.dot(ready[...], value_wide[...], preferred_element_type=F32)
    for h in range(2):
        flat[pl.ds(h, 256, stride=2), :] = wide[:, h * WIDTH:(h + 1) * WIDTH]
    for i in range(2):
        put_values(i, flat[pl.ds(i * 256, 256), :].astype(BF16))


def exchange_kernel(
    lat, rot, far_gain, key_up, value_up, keys, values, late, key_wide, value_wide, gain, pick,
    buf, stage, rot_raw, raw_w, flat,
    ready, load_sem, y_send, y_recv, z_send, z_recv, round_sem,
):
    me, z = lax.axis_index("span"), lax.axis_index("heads")
    ahead, behind = lax.rem(z + 1, RING), lax.rem(z + RING - 1, RING)

    sibling = target(me, 1)

    rot_load = pltpu.make_async_copy(rot, rot_raw, load_sem.at[0])
    rot_load.start()
    for t in range(TILES):
        rows = pl.ds(16 * (t // 4), 16)
        columns = pl.ds(128 * (t % 4), 128)
        pltpu.make_async_copy(
            lat.at[:, rows, columns], stage.at[:, t], load_sem.at[1]
        ).start()
    gain_load = pltpu.make_async_copy(far_gain, gain, load_sem.at[2])
    gain_load.start()
    for w, weight in enumerate((key_up, value_up)):
        pltpu.make_async_copy(weight, raw_w.at[w], load_sem.at[3]).start()

    barrier = pltpu.get_barrier_semaphore()
    greeted = [{"heads": near} for near in (ahead, behind)] + [{"span": target(me, k)} for k in range(1, NEAR)]
    greeted += [{"span": sibling, "heads": near} for near in (ahead, behind)]
    for device in greeted:
        pl.semaphore_signal(barrier, inc=1, device_id=device, device_id_type=MESH)

    rot_load.wait()
    for s in range(SPANS):
        part = rot_raw[s].astype(F32)
        stage[s, TILES] = jnp.concatenate([part[:16], part[16:]], axis=1).astype(BF16)

    all_rows = stage.at[:, pl.ds(0, TILES)]
    pltpu.make_async_copy(all_rows, all_rows, load_sem.at[1]).wait()
    pl.semaphore_wait(barrier, len(greeted))
    for near in (ahead, behind):
        pl.semaphore_signal(round_sem, inc=1, device_id={"heads": near}, device_id_type=MESH)

    def z_copy(way, d, ks):
        if way == 0:
            here, there, to = (RING + 1 - d) % RING, RING - d, ahead
        else:
            here, there, to = d - 1, d, behind
        places = pl.ds(ks[0], len(ks))
        src, device = buf.at[here, places], {"heads": to}
        if d == 1 and ks == (0,):
            src = stage.at[pl.ds(me, 1)]
        elif d == 1 and ks[0] < NEAR:
            to_span = target(me, ks[0])
            src, device = stage.at[pl.ds(to_span, 1)], {"span": to_span, "heads": to}
        return pltpu.make_async_remote_copy(
            src_ref=src, dst_ref=buf.at[there, places],
            send_sem=z_send.at[0], recv_sem=z_recv.at[Z_SEMS[way, d, ks[0]]],
            device_id=device, device_id_type=MESH,
        )

    def y_copy(k):
        to = target(me, k)
        return pltpu.make_async_remote_copy(
            src_ref=stage.at[pl.ds(to, 1)], dst_ref=buf.at[0, pl.ds(k, 1)],
            send_sem=y_send.at[0], recv_sem=y_recv.at[Y_SEMS[k]],
            device_id={"span": to}, device_id_type=MESH,
        )

    heard = set()

    def need(way, d, k):
        if d == 0:
            ks = y_unit(k)
            if ks != (0,) and (0, ks) not in heard:
                heard.add((0, ks))
                places = buf.at[0, pl.ds(ks[0], len(ks))]
                pltpu.make_async_remote_copy(
                    src_ref=places, dst_ref=places, send_sem=y_send.at[0],
                    recv_sem=y_recv.at[Y_SEMS[ks[0]]],
                    device_id={"span": sibling}, device_id_type=MESH,
                ).wait_recv()
            return
        ks = wait_unit(d, k)
        mark = (None if d == 4 else way, d, ks)
        if mark not in heard:
            heard.add(mark)
            places = buf.at[d if way else RING - d, pl.ds(ks[0], len(ks))]
            pltpu.make_async_remote_copy(
                src_ref=places, dst_ref=places, send_sem=z_send.at[0],
                recv_sem=z_recv.at[Z_SEMS[way, d, k]],
                device_id={"heads": ahead}, device_id_type=MESH,
            ).wait_recv()

    def forward(d, ks):
        for unit in dict.fromkeys(z_unit(d, k) for k in ks):
            for way in (0, 1):
                if d > 1 or unit[0] >= NEAR:
                    for k in unit:
                        need(way, d - 1, k)
                if d < 4 or way == last_way(unit[0]):
                    z_copy(way, d, unit).start()

    def spread(ks):
        for k in ks:
            y_copy(k).start()

    forward(1, [0, 1])
    spread(range(1, NEAR))
    buf[0, 0] = stage[me]

    gain_load.wait()
    pltpu.make_async_copy(raw_w, raw_w, load_sem.at[3]).wait()
    for w, put in ((0, key_wide), (1, value_wide)):
        @pl.loop(0, 4)
        def _(n):
            r = pl.multiple_of(n * 256, 256)
            flat[pl.ds(0, 256), :] = raw_w[w, pl.ds(r, 256), :].astype(F32)
            at = pl.multiple_of(n * 128, 128)
            for h in range(2):
                block = flat[pl.ds(h, 128, stride=2), :]
                if w == 0:
                    key_wide[h * WIDTH:(h + 1) * WIDTH, pl.ds(at, 128)] = block.T.astype(BF16)
                else:
                    value_wide[pl.ds(at, 128), h * WIDTH:(h + 1) * WIDTH] = block.astype(BF16)
    row = lax.broadcasted_iota(jnp.int32, (64, 128), 0)
    column = lax.broadcasted_iota(jnp.int32, (64, 128), 1)
    for half in range(2):
        place = (row // 16) * 32 + half * 16 + row % 16
        pick[half] = jnp.where(place == column, 1.0, 0.0).astype(BF16)

    def expand(p, other):
        group = z // 4 if not other else 1 - z // 4
        pair = (2 * p, 2 * p + 1)
        for k in pair:
            need(0, 0, k)
            for way in (0, 1):
                need(way, 3, k)
            if other:
                need(last_way(k), 4, k)
        rels = [lax.rem(group * 4 + zz + RING - z, RING) for zz in range(4)]
        if other and p == LAST:
            for i, k in enumerate(pair):
                for zz in range(4):
                    late[i, zz] = buf[rels[zz], k]
            return
        starts = [pl.multiple_of(source(me, k) * 256 + group * 128, 128) for k in pair]

        def put_keys(i, h, first, block):
            keys[h, first:first + block.shape[0], pl.ds(starts[i], 128)] = block

        def put_values(i, block):
            values[pl.ds(pl.multiple_of(starts[i] * 2, 256), 256), :] = block

        expand_pair(
            lambda i, zz, t: buf[rels[zz], pair[i], t],
            key_wide, value_wide, gain, pick, ready, flat, put_keys, put_values,
        )

    def hop(d, *pairs):
        for p in pairs:
            forward(d, [2 * p, 2 * p + 1])

    own, far = functools.partial(expand, other=False), functools.partial(expand, other=True)

    pl.semaphore_wait(round_sem, 2)
    forward(1, range(2, NEAR))
    forward(2, [0])
    for k in range(2, NEAR):
        need(0, 0, k)
    spread(range(NEAR, 10))
    forward(2, [1])
    hop(2, 1, 2)
    hop(1, 3, 4)
    spread(range(10, 16))
    hop(3, 0)
    hop(2, 3, 4)
    hop(3, 1)
    hop(1, 5, 6)
    hop(2, 5)
    own(0)
    hop(2, 6)
    hop(1, 7)
    hop(3, 2)
    hop(3, 3)
    own(1)
    hop(2, 7)
    hop(3, 4)
    hop(4, 0, 1)
    own(2)
    hop(3, 5)
    hop(3, 6)
    own(3)
    hop(3, 7)
    hop(4, 2, 3)
    own(4)
    far(0)
    far(1)
    hop(4, 4, 5)
    own(5)
    hop(4, 6, 7)
    own(6)
    own(7)
    for p in range(2, 8):
        far(p)
    for held, sem in ((buf.at[pl.ds(0, RING - 1)], z_send), (stage.at[pl.ds(0, SPANS - 1)], y_send)):
        pltpu.make_async_remote_copy(
            src_ref=held, dst_ref=held, send_sem=sem.at[0], recv_sem=y_recv.at[0],
            device_id={"span": sibling}, device_id_type=MESH,
        ).wait_send()


def write_kernel(
    keys_part, values_part, late, key_wide, value_wide, gain, pick, keys, values,
    ready, flat, keys_late, values_late, sem,
):
    me, z = lax.axis_index("span"), lax.axis_index("heads")
    near, away = z // 4, 1 - z // 4
    for k in range(SPANS):
        first, size = source(me, k) * 256, 256
        if k // 2 == LAST:
            first, size = first + near * 128, 128
        columns = pl.ds(pl.multiple_of(first, 128), size)
        rows = pl.ds(pl.multiple_of(first * 2, 256), size * 2)
        pltpu.make_async_copy(keys_part.at[:, :, columns], keys.at[0, :, :, columns], sem.at[0]).start()
        pltpu.make_async_copy(values_part.at[rows], values.at[rows], sem.at[1]).start()

    def put_keys(i, h, first, block):
        keys_late[i, h, first:first + block.shape[0], :] = block

    def put_values(i, block):
        values_late[i] = block

    expand_pair(
        lambda i, zz, t: late[i, zz, t],
        key_wide, value_wide, gain, pick, ready, flat, put_keys, put_values,
    )
    for i in range(2):
        first = source(me, 2 * LAST + i) * 256 + away * 128
        columns = pl.ds(pl.multiple_of(first, 128), 128)
        rows = pl.ds(pl.multiple_of(first * 2, 256), 256)
        pltpu.make_async_copy(keys_late.at[i], keys.at[0, :, :, columns], sem.at[2]).start()
        pltpu.make_async_copy(values_late.at[i], values.at[rows], sem.at[3]).start()
    length = keys_part.shape[2]
    early = (keys_part.at[:, :, pl.ds(0, length - 256)], values_part.at[pl.ds(0, 2 * length - 512)])
    for n, held in enumerate((*early, keys_late, values_late)):
        pltpu.make_async_copy(held, held, sem.at[n]).wait()


def shards(latents, rotary_rows, latent_gain, key_up, value_up):
    shape = (lax.axis_size("span"), lax.axis_size("heads"), *latents.shape, rotary_rows.shape[2])
    if shape != (SPANS, RING, SPANS, COUNT, DEPTH, TURN) or key_up.shape != (DEPTH, 2, WIDTH) or (
        value_up.shape != (DEPTH, 2, WIDTH)
    ):
        return plain_shards(latents, rotary_rows, latent_gain, key_up, value_up)
    length = SPANS * RING * COUNT
    near = pl.BlockSpec(memory_space=pltpu.VMEM)
    far = pl.BlockSpec(memory_space=pltpu.HBM)
    args = (
        latents, rotary_rows, latent_gain[None],
        key_up.reshape(2 * DEPTH, WIDTH), value_up.reshape(2 * DEPTH, WIDTH),
    )
    parts = pl.pallas_call(
        exchange_kernel,
        out_shape=(
            pltpu.VMEM((2, WIDTH + TURN, length), BF16),
            pltpu.VMEM((2 * length, WIDTH), BF16),
            pltpu.VMEM((2, 4, TILES + 1, 16, 128), BF16),
            pltpu.VMEM((2 * WIDTH, DEPTH), BF16),
            pltpu.VMEM((DEPTH, 2 * WIDTH), BF16),
            pltpu.VMEM((1, DEPTH), F32),
            pltpu.VMEM((2, 64, 128), BF16),
        ),
        in_specs=[far] * 5,
        out_specs=[near] * 7,
        scratch_shapes=[
            pltpu.VMEM((RING, SPANS, TILES + 1, 16, 128), BF16),
            pltpu.VMEM((SPANS, TILES + 1, 16, 128), BF16),
            pltpu.VMEM((SPANS, COUNT, TURN), BF16),
            pltpu.VMEM((2, 2 * DEPTH, WIDTH), BF16),
            pltpu.VMEM((512, WIDTH), F32),
            pltpu.VMEM((256, DEPTH), BF16),
            pltpu.SemaphoreType.DMA((4,)),
            pltpu.SemaphoreType.DMA((1,)),
            pltpu.SemaphoreType.DMA((Y_SEMS[SPANS - 1] + 1,)),
            pltpu.SemaphoreType.DMA((1,)),
            pltpu.SemaphoreType.DMA((len(set(Z_SEMS.values())),)),
            pltpu.SemaphoreType.REGULAR,
        ],
        compiler_params=pltpu.CompilerParams(
            collective_id=0, has_side_effects=True, vmem_limit_bytes=40 * 1024 * 1024
        ),
    )(*(pltpu.with_memory_space_constraint(arg, pltpu.HBM) for arg in args))
    keys, values = pl.pallas_call(
        write_kernel,
        out_shape=(
            jax.ShapeDtypeStruct((1, 2, WIDTH + TURN, length), BF16),
            jax.ShapeDtypeStruct((2 * length, WIDTH), BF16),
        ),
        in_specs=[near] * 7,
        out_specs=[far] * 2,
        scratch_shapes=[
            pltpu.VMEM((256, DEPTH), BF16),
            pltpu.VMEM((512, WIDTH), F32),
            pltpu.VMEM((2, 2, WIDTH + TURN, 128), BF16),
            pltpu.VMEM((2, 256, WIDTH), BF16),
            pltpu.SemaphoreType.DMA((4,)),
        ],
        compiler_params=pltpu.CompilerParams(vmem_limit_bytes=16 * 1024 * 1024),
    )(*parts)
    return keys, values.reshape(1, length, 2, WIDTH)


def solution(mesh):
    return jax.shard_map(
        shards,
        mesh=mesh,
        in_specs=(
            P("trial", ("span", "heads"), None),
            P("trial", ("span", "heads"), None),
            P(),
            P("trial", "heads", None),
            P("trial", "heads", None),
        ),
        out_specs=(
            P(("trial", "span"), "heads", None, None),
            P(("trial", "span"), None, "heads", None),
        ),
        check_vma=False,
    )
```
